32 devices in a mesh: task: 8 (over z, y), occ: 4 (over x, core).
Axes of the slice: x: 2, y: 2, z: 4, core: 2. Of those that a mesh axis runs over, the one named last changes fastest.
Arguments:
- ao_tiles: bfloat16 [1280, 8, 32, 128], P('task'), may hold values from -6 to 6
- mo_coeffs: bfloat16 [1536, 200], P(None, 'occ'), may hold values from -0.5 to 0.5
- mu_blocks: int32 [1280], P('task'), may hold values from 0 to 191
- nu_blocks: int32 [1280], P('task'), may hold values from 0 to 47
- tile_live: int32 [1280], P('task'), may hold values 0 or 1
- batch_target: int32 [160], P('task'), may hold values from 0 to 2
- batch_count: int32 [8], P('task'), may hold values from 1 to 20
Outputs:
- half_mo: float32 [200, 200, 1024], P('occ', None, 'task')
The draws below stay inside these ranges and needn't reach their ends.
Inputs may be any that keep to these rules, and one draw needn't show every extreme that they name: `batch_target`: the batch's kl block is the block owned by task index (own index + value) mod 8. `batch_count`: batches at or after this count in a list are not part of the work.
All inputs are finite; a program needn't handle non-finite values. No bound on the sum of `tile_live` on one device may be relied on, other than what follows from the above.
Results may differ from the reference program's by a relative error of at most 0.0029.
Values may be sent and summed in bfloat16 or wider, within the bound.
A program may use at most 128 MiB of HBM per device.

```python
import jax
import jax.numpy as jnp
from jax import lax

NBF = 1536
NOCC = 200
MUT = 8
NUT = 32
KLW = 128
BATCH = 8
NB = 20
SPREAD = 3
BLOCKS = 160
TILES = 1280
N_TASK = 8


def with_ends(result, rng, smallest, largest):
    index_at = [jax.random.randint(jax.random.fold_in(rng, axis), (), 0, length) for axis, length in enumerate(result.shape)]
    widest = result.shape.index(max(result.shape))
    neighbour = index_at[:widest] + [(index_at[widest] + 1) % result.shape[widest]] + index_at[widest + 1:]
    return result.at[tuple(index_at)].set(smallest).at[tuple(neighbour)].set(largest)


def steps_of(own_key, shape, cuts, least, high):
    gain, own = 1.0, jax.random.fold_in(own_key, 6)
    for dim, shards_of in cuts:
        heights = jnp.exp(jax.random.uniform(jax.random.fold_in(own, dim), (shards_of,), jnp.float32, least / len(cuts), high / len(cuts)))
        gain = gain * jnp.repeat(heights, shape[dim] // shards_of).reshape([-1 if axis == dim else 1 for axis in range(len(shape))])
    return gain


def scatter_about(own_key, dims, spread, reach, split=(), held_as=jnp.bfloat16):
    level = steps_of(own_key, dims, split, -0.22, 0.18) if split else 1.0
    array = jax.random.normal(own_key, dims, jnp.float32) * spread * level
    return jnp.minimum(jnp.maximum(array, -reach), reach).astype(held_as)


def setup_inputs(seed: int = 0) -> dict:
    key_list = jax.random.split(jax.random.key(seed), 8)
    return {
        "ao_tiles": scatter_about(key_list[0], (TILES, MUT, NUT, KLW), 1.0, 6.0, ((0, 8),)),
        "mo_coeffs": scatter_about(key_list[1], (NBF, NOCC), 128 ** -0.5, 0.5, ((1, 4),)),
        "mu_blocks": with_ends(jax.random.randint(key_list[2], (TILES,), 0, NBF // MUT), jax.random.fold_in(key_list[2], 1), 0, (NBF // MUT) - 1).astype(jnp.int32),
        "nu_blocks": with_ends(jax.random.randint(key_list[3], (TILES,), 0, NBF // NUT), jax.random.fold_in(key_list[3], 1), 0, (NBF // NUT) - 1).astype(jnp.int32),
        "tile_live": with_ends((jax.random.randint(key_list[4], (TILES,), 0, 4) < 3).astype(jnp.int32), jax.random.fold_in(key_list[4], 1), 0, 1),
        "batch_target": with_ends(jax.random.randint(key_list[5], (BLOCKS,), 0, SPREAD), jax.random.fold_in(key_list[5], 1), 0, SPREAD - 1).astype(jnp.int32),
        "batch_count": with_ends(jax.random.randint(key_list[6], (N_TASK,), 1, NB + 1), jax.random.fold_in(key_list[6], 1), 1, NB).astype(jnp.int32),
    }


def reference(ao_tiles, mo_coeffs, mu_blocks, nu_blocks, tile_live, batch_target, batch_count):
    coeff_full = mo_coeffs.astype(jnp.float32)
    tiles_all = ao_tiles.reshape(N_TASK, NB, BATCH, MUT, NUT, KLW)
    mu_all = mu_blocks.reshape(N_TASK, NB, BATCH)
    nu_all = nu_blocks.reshape(N_TASK, NB, BATCH)
    live_all = tile_live.reshape(N_TASK, NB, BATCH)
    target_all = batch_target.reshape(N_TASK, NB)
    mu_offsets = jnp.arange(MUT, dtype=jnp.int32)
    nu_offsets = jnp.arange(NUT, dtype=jnp.int32)
    spread_ids = jnp.arange(SPREAD, dtype=jnp.int32)

    def one_group(output, group_items):
        tiles_g, mu_g, nu_g, live_g, target_g, listed, group_index = group_items

        def one_batch(partials, batch_items):
            tile_block, mu_ids, nu_ids, live_ids, target, batch_index = batch_items
            coeff_mu = coeff_full[mu_ids[:, None] * MUT + mu_offsets[None, :]]
            quarter = jnp.einsum("bmi,bmnk->bink", coeff_mu, tile_block.astype(jnp.float32)).astype(jnp.bfloat16)
            kept_tiles = (live_ids * (batch_index < listed).astype(jnp.int32)).astype(jnp.float32)
            coeff_nu = coeff_full[nu_ids[:, None] * NUT + nu_offsets[None, :]] * kept_tiles[:, None, None]
            contribution = jnp.einsum("bnj,bink->ijk", coeff_nu, quarter.astype(jnp.float32))
            chosen = (spread_ids == target).astype(jnp.float32)
            return partials + chosen[:, None, None, None] * contribution[None], None

        initial = jnp.zeros((SPREAD, NOCC, NOCC, KLW), jnp.float32)
        partials = lax.scan(one_batch, initial, (tiles_g, mu_g, nu_g, live_g, target_g, jnp.arange(NB, dtype=jnp.int32)))[0]
        for spread_index in range(SPREAD):
            owner_index = (group_index + spread_index) % N_TASK
            column = (owner_index * KLW).astype(jnp.int32)
            earlier = lax.dynamic_slice_in_dim(output, column, KLW, 2)
            output = lax.dynamic_update_slice_in_dim(output, earlier + partials[spread_index], column, 2)
        return output, None

    output = jnp.zeros((NOCC, NOCC, N_TASK * KLW), jnp.float32)
    output = lax.scan(one_group, output, (tiles_all, mu_all, nu_all, live_all, target_all, batch_count, jnp.arange(N_TASK, dtype=jnp.int32)))[0]
    return output
```

```python
from functools import partial

import jax
import jax.numpy as jnp
from jax import lax
from jax.experimental import pallas as pl
from jax.experimental.pallas import tpu as pltpu
from jax.sharding import PartitionSpec as P

SPREAD = 3
GROUP = 8
F32 = jnp.float32
BF16 = jnp.bfloat16


def plan_kernel(live_ref, target_ref, count_ref, slots_ref, filled_ref):
    per_batch = live_ref.shape[0] // target_ref.shape[0]
    room = live_ref.shape[0] + GROUP
    for s in range(SPREAD):
        filled_ref[s] = 0

    def take_batch(batch, carry):
        target = target_ref[batch]
        at = filled_ref[target]
        for q in range(per_batch):
            tile = batch * per_batch + q
            slots_ref[target * room + at] = tile
            at = at + live_ref[tile]
        filled_ref[target] = at
        return carry

    lax.fori_loop(0, count_ref[0], take_batch, 0)
    for s in range(SPREAD):
        end = filled_ref[s]
        for q in range(GROUP):
            slots_ref[s * room + end + q] = 0


def make_plan(tile_live, batch_target, batch_count):
    smem = pl.BlockSpec(memory_space=pltpu.SMEM)
    room = tile_live.shape[0] + GROUP
    return pl.pallas_call(
        plan_kernel,
        out_shape=(
            jax.ShapeDtypeStruct((SPREAD * room,), jnp.int32),
            jax.ShapeDtypeStruct((SPREAD,), jnp.int32),
        ),
        in_specs=[smem] * 3,
        out_specs=(smem, smem),
        name="plan",
    )(tile_live, batch_target, batch_count)


def contract_kernel(targets, room, slots_ref, filled_ref, mu_ref, nu_ref, tiles, *refs):
    coeff_i, coeff_all, pick, own, interleave, unit = refs[:6]
    outs = refs[6 : 6 + len(targets)]
    held, turned, quarter, total, landed = refs[6 + len(targets) :]
    _, mu_width, nu_width, kl = tiles.shape
    occ = total.shape[0]
    depth = GROUP * mu_width
    across = (((1,), (1,)), ((), ()))

    def fetch(target, group, slot):
        return [
            pltpu.make_async_copy(
                tiles.at[slots_ref[target * room + group * GROUP + b]], held.at[slot, b], landed.at[slot]
            )
            for b in range(GROUP)
        ]

    def visit(target, groups, group, slot):
        for copy in fetch(target, group, slot):
            copy.wait()

        @pl.when(group + 1 < groups)
        def _():
            for copy in fetch(target, group + 1, 1 - slot):
                copy.start()

        for b in range(GROUP):
            for m in range(mu_width):
                turned[pl.ds(b * mu_width + m, nu_width, stride=depth), :] = held[slot, b, m].astype(F32)

        mus, nus = [], []
        for b in range(GROUP):
            place = group * GROUP + b
            tile = slots_ref[target * room + place]
            mus.append(coeff_i[mu_ref[tile]])
            rows = coeff_all[pl.ds(pl.multiple_of(nu_ref[tile] * nu_width, nu_width), nu_width), :]
            nus.append(rows.astype(F32) * jnp.where(place < filled_ref[target], 1.0, 0.0))
        mu_rows = jnp.concatenate(mus, axis=0).astype(BF16)
        nu_rows = jnp.concatenate(nus, axis=0).astype(BF16)
        left = lax.dot_general(pick[...], mu_rows, across, preferred_element_type=F32)
        left = (left * own[...]).astype(BF16)
        mixed = jnp.dot(interleave[...], nu_rows, preferred_element_type=F32).astype(BF16)
        right = lax.dot_general(unit[...], mixed, across, preferred_element_type=F32).astype(BF16)

        for p in range(nu_width // 2):
            even, later = 2 * p * depth, (2 * p + 1) * depth
            pair = jnp.concatenate(
                [turned[even : even + depth, :], turned[later : later + depth, :]], axis=1
            ).astype(BF16)
            got = jnp.dot(left, pair, preferred_element_type=F32).reshape(occ, GROUP, 2 * kl)
            got = jnp.concatenate([got[:, :, :kl], got[:, :, kl:]], axis=1)
            quarter[:, 2 * p * GROUP : (2 * p + 2) * GROUP, :] = got.astype(BF16)

        for h in range(occ // 2):
            both = jnp.concatenate([quarter[2 * h], quarter[2 * h + 1]], axis=1)
            got = jnp.dot(right, both, preferred_element_type=F32)
            total[2 * h] += got[:, :kl]
            total[2 * h + 1] += got[:, kl:]
        if occ % 2:
            total[occ - 1] += jnp.dot(right, quarter[occ - 1], preferred_element_type=F32)
        return 1 - slot

    for target, out in zip(targets, outs):
        groups = lax.div(filled_ref[target] + (GROUP - 1), GROUP)
        total[...] = jnp.zeros_like(total)

        @pl.when(groups > 0)
        def _(target=target):
            for copy in fetch(target, 0, 0):
                copy.start()

        lax.fori_loop(0, groups, lambda g, slot, t=target, n=groups: visit(t, n, g, slot), jnp.int32(0))
        out[...] = total[...].astype(out.dtype)


def contract(targets, dtype, start, occ, ao_tiles, coeff_i, coeff_all, plan, mu_blocks, nu_blocks):
    slots, filled = plan
    count, mu_width, nu_width, kl = ao_tiles.shape
    all_occ = coeff_all.shape[1]
    local_occ = coeff_i.shape[2]
    room = count + GROUP
    depth, width = GROUP * mu_width, GROUP * nu_width

    def eq(rows, columns):
        return rows[:, None] == columns[None, :]

    out_rows = jnp.arange(occ * GROUP)
    pick = eq(out_rows // GROUP + start, jnp.arange(local_occ)).astype(BF16)
    own = eq(out_rows % GROUP, jnp.arange(depth) // mu_width).astype(F32)
    mixed_rows = jnp.arange(width)
    interleave = eq(mixed_rows % GROUP * nu_width + mixed_rows // GROUP, mixed_rows).astype(BF16)
    unit = eq(jnp.arange(all_occ), jnp.arange(all_occ)).astype(BF16)
    shared = [coeff_i, coeff_all, pick, own, interleave, unit]
    share = occ * len(targets) * max(1, count // GROUP // SPREAD)
    outs = [jax.ShapeDtypeStruct((occ, all_occ, kl), dtype) for _ in targets]
    return pl.pallas_call(
        partial(contract_kernel, targets, room),
        out_shape=outs,
        in_specs=[pl.BlockSpec(memory_space=pltpu.SMEM)] * 4
        + [pl.BlockSpec(memory_space=pl.ANY)]
        + [pl.BlockSpec(memory_space=pltpu.VMEM)] * len(shared),
        out_specs=[pl.BlockSpec(memory_space=pltpu.VMEM) for _ in targets],
        scratch_shapes=[
            pltpu.VMEM((2, GROUP, mu_width, nu_width, kl), BF16),
            pltpu.VMEM((nu_width * depth, kl), F32),
            pltpu.VMEM((occ, width, kl), BF16),
            pltpu.VMEM((occ, all_occ, kl), F32),
            pltpu.SemaphoreType.DMA((2,)),
        ],
        compiler_params=pltpu.CompilerParams(vmem_limit_bytes=56 * 1024 * 1024),
        cost_estimate=pl.CostEstimate(
            flops=4 * share * all_occ * width * kl, bytes_accessed=share * all_occ * kl, transcendentals=0
        ),
        name="contract",
    )(slots, filled, mu_blocks, nu_blocks, ao_tiles, *shared)


def local(ao_tiles, mo_coeffs, mu_blocks, nu_blocks, tile_live, batch_target, batch_count):
    mu_width = ao_tiles.shape[1]
    local_occ = mo_coeffs.shape[1]
    plan = make_plan(tile_live, batch_target, batch_count)
    coeff_all = lax.all_gather(mo_coeffs, "occ", axis=1, tiled=True)
    coeff_i = mo_coeffs.astype(F32).reshape(-1, mu_width, local_occ)
    tasks = lax.axis_size("task")
    swap = [(t, t ^ 1) for t in range(tasks)]
    ahead = [(t, (t + 2) % tasks) for t in range(tasks)]
    odd = lax.axis_index("task") % 2 == 1

    pieces = next(n for n in range(min(5, local_occ), 0, -1) if local_occ % n == 0)
    occ = local_occ // pieces
    work = (ao_tiles, coeff_i, coeff_all, plan, mu_blocks, nu_blocks)
    swapped, arrived = [], []
    for c in range(pieces):
        one, two = contract((1, 2), BF16, c * occ, occ, *work)
        other = lax.ppermute(one, "task", swap)
        send = jnp.where(odd, two, (two.astype(F32) + other.astype(F32)).astype(BF16))
        arrived.append(lax.ppermute(send, "task", ahead))
        swapped.append(other)
    (result,) = contract((0,), F32, 0, local_occ, *work)
    for c in range(pieces):
        part = lax.slice_in_dim(result, c * occ, (c + 1) * occ, axis=0)
        part = part + (arrived[c].astype(F32) + jnp.where(odd, swapped[c].astype(F32), 0.0))
        result = lax.dynamic_update_slice_in_dim(result, part, c * occ, axis=0)
    return result


def solution(mesh):
    in_specs = (
        P("task", None, None, None),
        P(None, "occ"),
        P("task"),
        P("task"),
        P("task"),
        P("task"),
        P("task"),
    )
    out_specs = P("occ", None, "task")
    return jax.shard_map(local, mesh=mesh, in_specs=in_specs, out_specs=out_specs, check_vma=False)
```

```python
from functools import partial

import jax
import jax.numpy as jnp
import numpy as np
from jax import lax
from jax.experimental import pallas as pl
from jax.experimental.pallas import tpu as pltpu
from jax.sharding import PartitionSpec as P

SPREAD = 3
GROUP = 8
F32 = jnp.float32
BF16 = jnp.bfloat16


def plan_kernel(live_ref, target_ref, count_ref, slots_ref, filled_ref):
    per_batch = live_ref.shape[0] // target_ref.shape[0]
    room = live_ref.shape[0] + GROUP
    for s in range(SPREAD):
        filled_ref[s] = 0

    def take_batch(batch, carry):
        target = target_ref[batch]
        at = filled_ref[target]
        for q in range(per_batch):
            tile = batch * per_batch + q
            slots_ref[target * room + at] = tile
            at = at + live_ref[tile]
        filled_ref[target] = at
        return carry

    lax.fori_loop(0, count_ref[0], take_batch, 0)
    for s in range(SPREAD):
        end = filled_ref[s]
        for q in range(GROUP):
            slots_ref[s * room + end + q] = 0


def make_plan(tile_live, batch_target, batch_count):
    smem = pl.BlockSpec(memory_space=pltpu.SMEM)
    room = tile_live.shape[0] + GROUP
    return pl.pallas_call(
        plan_kernel,
        out_shape=(
            jax.ShapeDtypeStruct((SPREAD * room,), jnp.int32),
            jax.ShapeDtypeStruct((SPREAD,), jnp.int32),
        ),
        in_specs=[smem] * 3,
        out_specs=(smem, smem),
        name="plan",
    )(tile_live, batch_target, batch_count)


def contract_kernel(targets, pieces, room, slots_ref, filled_ref, mu_ref, nu_ref, tiles, *refs):
    coeff_i, coeff_all, pick, own, interleave, unit = refs[:6]
    outs = refs[6 : 6 + len(targets) * pieces]
    held, turned, quarter, total, landed = refs[6 + len(targets) * pieces :]
    _, mu_width, nu_width, kl = tiles.shape
    occ = total.shape[0]
    depth = GROUP * mu_width
    across = (((1,), (1,)), ((), ()))

    def fetch(target, group, slot):
        return [
            pltpu.make_async_copy(
                tiles.at[slots_ref[target * room + group * GROUP + b]], held.at[slot, b], landed.at[slot]
            )
            for b in range(GROUP)
        ]

    def visit(target, groups, group, slot):
        for copy in fetch(target, group, slot):
            copy.wait()

        @pl.when(group + 1 < groups)
        def _():
            for copy in fetch(target, group + 1, 1 - slot):
                copy.start()

        for b in range(GROUP):
            for m in range(mu_width):
                turned[pl.ds(b * mu_width + m, nu_width, stride=depth), :] = held[slot, b, m].astype(F32)

        mus, nus = [], []
        for b in range(GROUP):
            place = group * GROUP + b
            tile = slots_ref[target * room + place]
            mus.append(coeff_i[mu_ref[tile]])
            rows = coeff_all[pl.ds(pl.multiple_of(nu_ref[tile] * nu_width, nu_width), nu_width), :]
            nus.append(rows.astype(F32) * jnp.where(place < filled_ref[target], 1.0, 0.0))
        mu_rows = jnp.concatenate(mus, axis=0).astype(BF16)
        nu_rows = jnp.concatenate(nus, axis=0).astype(BF16)
        left = lax.dot_general(pick[...], mu_rows, across, preferred_element_type=F32)
        left = (left * own[...]).astype(BF16)
        mixed = jnp.dot(interleave[...], nu_rows, preferred_element_type=F32).astype(BF16)
        right = lax.dot_general(unit[...], mixed, across, preferred_element_type=F32).astype(BF16)

        for p in range(nu_width // 2):
            even, later = 2 * p * depth, (2 * p + 1) * depth
            pair = jnp.concatenate(
                [turned[even : even + depth, :], turned[later : later + depth, :]], axis=1
            ).astype(BF16)
            got = jnp.dot(left, pair, preferred_element_type=F32).reshape(occ, GROUP, 2 * kl)
            got = jnp.concatenate([got[:, :, :kl], got[:, :, kl:]], axis=1)
            quarter[:, 2 * p * GROUP : (2 * p + 2) * GROUP, :] = got.astype(BF16)

        for h in range(occ // 2):
            both = jnp.concatenate([quarter[2 * h], quarter[2 * h + 1]], axis=1)
            got = jnp.dot(right, both, preferred_element_type=F32)
            total[2 * h] += got[:, :kl]
            total[2 * h + 1] += got[:, kl:]
        if occ % 2:
            total[occ - 1] += jnp.dot(right, quarter[occ - 1], preferred_element_type=F32)
        return 1 - slot

    for k, target in enumerate(targets):
        groups = lax.div(filled_ref[target] + (GROUP - 1), GROUP)
        total[...] = jnp.zeros_like(total)

        @pl.when(groups > 0)
        def _(target=target):
            for copy in fetch(target, 0, 0):
                copy.start()

        lax.fori_loop(0, groups, lambda g, slot, t=target, n=groups: visit(t, n, g, slot), jnp.int32(0))
        part = occ // pieces
        for c, out in enumerate(outs[k * pieces : (k + 1) * pieces]):
            out[...] = total[c * part : (c + 1) * part].astype(out.dtype)


def contract(targets, dtype, pieces, ao_tiles, coeff_i, coeff_all, plan, mu_blocks, nu_blocks):
    slots, filled = plan
    count, mu_width, nu_width, kl = ao_tiles.shape
    all_occ = coeff_all.shape[1]
    occ = coeff_i.shape[2]
    room = count + GROUP
    depth, width = GROUP * mu_width, GROUP * nu_width

    def eq(rows, columns, dtype=BF16):
        return jnp.asarray(rows[:, None] == columns[None, :], dtype)

    out_rows = np.arange(occ * GROUP)
    pick = eq(out_rows // GROUP, np.arange(occ))
    own = eq(out_rows % GROUP, np.arange(depth) // mu_width, F32)
    mixed_rows = np.arange(width)
    interleave = eq(mixed_rows % GROUP * nu_width + mixed_rows // GROUP, mixed_rows)
    unit = eq(np.arange(all_occ), np.arange(all_occ))
    shared = [coeff_i, coeff_all, pick, own, interleave, unit]
    share = occ * len(targets) * max(1, count // GROUP // SPREAD)
    outs = [jax.ShapeDtypeStruct((occ // pieces, all_occ, kl), dtype)] * (len(targets) * pieces)
    return pl.pallas_call(
        partial(contract_kernel, targets, pieces, room),
        out_shape=outs,
        in_specs=[pl.BlockSpec(memory_space=pltpu.SMEM)] * 4
        + [pl.BlockSpec(memory_space=pl.ANY)]
        + [pl.BlockSpec(memory_space=pltpu.VMEM)] * len(shared),
        out_specs=[pl.BlockSpec(memory_space=pltpu.VMEM)] * len(outs),
        scratch_shapes=[
            pltpu.VMEM((2, GROUP, mu_width, nu_width, kl), BF16),
            pltpu.VMEM((nu_width * depth, kl), F32),
            pltpu.VMEM((occ, width, kl), BF16),
            pltpu.VMEM((occ, all_occ, kl), F32),
            pltpu.SemaphoreType.DMA((2,)),
        ],
        compiler_params=pltpu.CompilerParams(vmem_limit_bytes=56 * 1024 * 1024),
        cost_estimate=pl.CostEstimate(
            flops=4 * share * all_occ * width * kl, bytes_accessed=share * all_occ * kl, transcendentals=0
        ),
        name="contract",
    )(slots, filled, mu_blocks, nu_blocks, ao_tiles, *shared)


def local(ao_tiles, mo_coeffs, mu_blocks, nu_blocks, tile_live, batch_target, batch_count):
    mu_width = ao_tiles.shape[1]
    local_occ = mo_coeffs.shape[1]
    plan = make_plan(tile_live, batch_target, batch_count)
    coeff_all = lax.all_gather(mo_coeffs, "occ", axis=1, tiled=True)
    coeff_i = mo_coeffs.astype(F32).reshape(-1, mu_width, local_occ)
    tasks = lax.axis_size("task")
    swap = [(t, t ^ 1) for t in range(tasks)]
    ahead = [(t, (t + 2) % tasks) for t in range(tasks)]
    odd = lax.axis_index("task") % 2 == 1

    pieces = next(n for n in range(min(10, local_occ), 0, -1) if local_occ % n == 0)
    occ = local_occ // pieces
    work = (ao_tiles, coeff_i, coeff_all, plan, mu_blocks, nu_blocks)
    sums = contract((1, 2), BF16, pieces, *work)
    swapped = [lax.ppermute(one, "task", swap) for one in sums[:pieces]]
    arrived = []
    for two, other in zip(sums[pieces:], swapped):
        send = jnp.where(odd, two, (two.astype(F32) + other.astype(F32)).astype(BF16))
        arrived.append(lax.ppermute(send, "task", ahead))
    (result,) = contract((0,), F32, 1, *work)
    for c in range(pieces):
        part = lax.slice_in_dim(result, c * occ, (c + 1) * occ, axis=0)
        part = part + (arrived[c].astype(F32) + jnp.where(odd, swapped[c].astype(F32), 0.0))
        result = lax.dynamic_update_slice_in_dim(result, part, c * occ, axis=0)
    return result


def solution(mesh):
    in_specs = (
        P("task", None, None, None),
        P(None, "occ"),
        P("task"),
        P("task"),
        P("task"),
        P("task"),
        P("task"),
    )
    out_specs = P("occ", None, "task")
    return jax.shard_map(local, mesh=mesh, in_specs=in_specs, out_specs=out_specs, check_vma=False)
```
